512 devices in a mesh: row: 32 (over x, y, core), col: 16 (over z).
Axes of the slice: x: 4, y: 4, z: 16, core: 2. Of those that a mesh axis runs over, the one named last changes fastest.
Arguments:
- right_side: float32 [5, 32, 16, 32, 128], P(None, 'row', 'col'), may hold values from -6 to 6
- diag_blocks: float32 [5, 32, 16, 128, 128], P(None, 'row', 'col'), may hold values from -1 to 2, as said below
- off_blocks: float32 [32, 16, 4, 8, 128, 128], P('row', 'col'), may hold values from -0.1875 to 0.1875
- slot_target: int32 [32, 16, 4, 8], P('row', 'col'), may hold values from 0 to 31
- slot_level: int32 [32, 16, 4, 8], P('row', 'col'), may hold values from 0 to 3, as said below
- slot_position: int32 [32, 16, 4, 8], P('row', 'col'), may hold values from 0 to 15
- slot_count: int32 [32, 16, 4], P('row', 'col'), may hold values from 1 to 8
Outputs:
- solution: float32 [5, 32, 16, 32, 128], P(None, 'row', 'col')
The draws below stay inside these ranges and needn't reach their ends.
Inputs may be any that keep to these rules, and one draw needn't show every extreme that they name: slot_level[..., m, s] is a level below the target level m + 1. slot_target names a row group. slot_position names a column group. `diag_blocks`: each diagonal block is lower triangular with its diagonal between 1 and 2 and strictly lower entries of size at most 1 / sqrt(128).
All inputs are finite; a program needn't handle non-finite values.
Results may differ from the reference program's by a relative error of at most 0.0001.
Values sent between devices are 32-bit elements; how exact they have to be, the bound alone decides.
No kernel may reach another device: no remote copies, remote signals or barrier semaphores. Data moves between devices by JAX's collectives and lax.ppermute only.
A program may use at most 64 MiB of HBM per device.

```python
import math
import jax
import jax.numpy as jnp
from jax import lax

B = 128
NRHS = 32
LEVELS = 5
SLOTS = 8
GRID_ROWS = 32
GRID_COLS = 16


def draw_diag_blocks(key, part):
    first_key, second_key, third_key = jax.random.split(key, 3)
    shape_all = (LEVELS, GRID_ROWS, GRID_COLS, B, B)
    limit = 1.0 / math.sqrt(B)
    strict = jax.random.uniform(first_key, shape_all, jnp.float32, -limit, limit)
    main = jax.random.uniform(second_key, shape_all[:-1], jnp.float32, 1.0, 2.0)
    matrix = jnp.tril(strict, -1) + main[..., None] * jnp.eye(B, dtype=jnp.float32)
    return matrix.astype(jnp.float32)


def draw_slot_level(key, part):
    bounds = jnp.arange(1, LEVELS, dtype=jnp.int32)[None, None, :, None]
    raw_bits = jax.random.randint(key, (GRID_ROWS, GRID_COLS, LEVELS - 1, SLOTS), 0, 1 << 20, dtype=jnp.int32)
    return (raw_bits % bounds).astype(jnp.int32)


def with_ends(array, key, low, top_value):
    extent = array.shape
    index_at = [jax.random.randint(jax.random.fold_in(key, axis), (), 0, extent[axis]) for axis in range(len(extent))]
    array = array.at[tuple(index_at)].set(low)
    longest = extent.index(max(extent))
    index_at[longest] = (index_at[longest] + 1) % extent[longest]
    return array.at[tuple(index_at)].set(top_value)


def levels(rng, dims, cuts, smallest, top_value):
    gain = 1.0
    for dim, parts in cuts:
        heights = jax.random.uniform(jax.random.fold_in(jax.random.fold_in(rng, 6), dim), (parts,), jnp.float32, smallest / len(cuts), top_value / len(cuts))
        gain = gain * jnp.repeat(jnp.exp(heights), dims[dim] // parts).reshape((-1,) + (1,) * (len(dims) - 1 - dim))
    return gain


def noise(stream_key, extent, scale, most, pieces=(), held_as=jnp.bfloat16):
    drawn = jax.random.normal(stream_key, extent, jnp.float32) * scale
    if len(pieces) > 0:
        drawn = levels(stream_key, extent, pieces, -0.22, 0.18) * drawn
    return jnp.clip(drawn, min=-most, max=most).astype(held_as)


def setup_inputs(seed: int = 0) -> dict:
    splits = jax.random.split(jax.random.key(seed), 8)
    return {
        "right_side": noise(splits[0], (LEVELS, GRID_ROWS, GRID_COLS, NRHS, B), 1.0, 6.0, ((1, 32), (2, 16)), jnp.float32),
        "diag_blocks": draw_diag_blocks(jax.random.fold_in(splits[7], 71), 0),
        "off_blocks": noise(splits[2], (GRID_ROWS, GRID_COLS, LEVELS - 1, SLOTS, B, B), (B * SLOTS) ** -0.5, 0.1875, ((0, 32), (1, 16)), jnp.float32),
        "slot_target": with_ends(jax.random.randint(splits[3], (GRID_ROWS, GRID_COLS, LEVELS - 1, SLOTS), 0, GRID_ROWS), jax.random.fold_in(splits[3], 1), 0, GRID_ROWS - 1).astype(jnp.int32),
        "slot_level": draw_slot_level(jax.random.fold_in(splits[7], 71), 0),
        "slot_position": with_ends(jax.random.randint(splits[5], (GRID_ROWS, GRID_COLS, LEVELS - 1, SLOTS), 0, GRID_COLS), jax.random.fold_in(splits[5], 1), 0, GRID_COLS - 1).astype(jnp.int32),
        "slot_count": with_ends(jax.random.randint(splits[6], (GRID_ROWS, GRID_COLS, LEVELS - 1), 1, SLOTS + 1), jax.random.fold_in(splits[6], 1), 1, SLOTS).astype(jnp.int32),
    }


def solve_block(diagonal, right_rows):
    return jax.scipy.linalg.solve_triangular(diagonal, right_rows.T, lower=True).T

def reference(right_side, diag_blocks, off_blocks, slot_target, slot_level, slot_position, slot_count):
    solver = jax.vmap(jax.vmap(solve_block))
    solved = [solver(diag_blocks[0], right_side[0])]
    row_index = jnp.arange(GRID_ROWS, dtype=jnp.int32)[:, None, None]
    slot_ids = jnp.arange(SLOTS, dtype=jnp.int32)
    group_ids = jnp.arange(GRID_ROWS, dtype=jnp.int32)
    for level_now in range(1, LEVELS):
        source_tier = level_now - 1
        gathered = jnp.stack(solved)
        operands = gathered[slot_level[:, :, source_tier], row_index, slot_position[:, :, source_tier]]
        active = (slot_ids[None, None, :] < slot_count[:, :, source_tier:source_tier + 1]).astype(jnp.float32)
        products = jnp.einsum('rcsnb,rcsab->rcsna', operands, off_blocks[:, :, source_tier], precision=lax.Precision.HIGHEST)
        products = products * active[:, :, :, None, None]
        selector = (slot_target[:, :, source_tier][..., None] == group_ids).astype(jnp.float32)
        coupling = jnp.einsum('rcst,rcsna->tcna', selector, products, precision=lax.Precision.HIGHEST)
        solved.append(solver(diag_blocks[level_now], right_side[level_now] - coupling))
    return jnp.stack(solved)
```

```python
import functools

import jax
import jax.numpy as jnp
from jax import lax
from jax.experimental import pallas as pl
from jax.experimental.pallas import tpu as pltpu
from jax.sharding import PartitionSpec as P

HIGHEST = lax.Precision.HIGHEST
VMEM = pltpu.VMEM
SMEM = pltpu.SMEM
BASE = 32


def mm(a, b):
    return jnp.dot(a, b, precision=HIGHEST, preferred_element_type=jnp.float32)


def mm_nt(a, b):
    return lax.dot_general(
        a, b, (((1,), (1,)), ((), ())), precision=HIGHEST, preferred_element_type=jnp.float32
    )


def invert_lower(blocks):
    size = blocks[0].shape[0]
    rows = lax.broadcasted_iota(jnp.int32, (size, size), 0)
    cols = lax.broadcasted_iota(jnp.int32, (size, size), 1)
    eye = rows == cols
    strict = rows > cols
    same = (rows // BASE) == (cols // BASE)
    scaled, scale_cols, powers, inverses = [], [], [], []
    for block in blocks:
        on_diag = jnp.where(eye, block, 0.0)
        scale_rows = 1.0 / jnp.sum(on_diag, axis=1, keepdims=True)
        scale_cols.append(1.0 / jnp.sum(on_diag, axis=0, keepdims=True))
        m = jnp.where(strict, block * scale_rows, 0.0)
        scaled.append(m)
        local = jnp.where(same, m, 0.0)
        powers.append(local)
        inverses.append(jnp.where(eye, 1.0, 0.0) - local)
    span = 2
    while span < BASE:
        powers = [mm(p, p) for p in powers]
        inverses = [v + mm(v, p) for v, p in zip(inverses, powers)]
        span *= 2
    width = BASE
    while width < size:
        joins = ((rows // (2 * width)) == (cols // (2 * width))) & (
            (rows // width) > (cols // width)
        )
        steps = [mm(jnp.where(joins, m, 0.0), v) for m, v in zip(scaled, inverses)]
        inverses = [v - mm(v, s) for v, s in zip(inverses, steps)]
        width *= 2
    return [v * s for v, s in zip(inverses, scale_cols)]


def first_kernel(diag_ref, right_ref, solved_ref, copies_ref):
    (inverse,) = invert_lower([diag_ref[...]])
    solved = mm_nt(right_ref[...], inverse)
    solved_ref[...] = solved
    for peer in range(copies_ref.shape[0]):
        copies_ref[peer] = solved


def invert_kernel(diag_ref, inverse_ref):
    count = diag_ref.shape[0]
    for at, inverse in enumerate(invert_lower([diag_ref[i] for i in range(count)])):
        inverse_ref[at] = inverse


def reduced_solve(received_ref, right_ref, inverse_ref):
    total = received_ref[0]
    for peer in range(1, received_ref.shape[0]):
        total = total + received_ref[peer]
    return mm_nt(right_ref[...] - total, inverse_ref[...])


def solve_kernel(received_ref, right_ref, inverse_ref, solved_ref, copies_ref):
    solved = reduced_solve(received_ref, right_ref, inverse_ref)
    solved_ref[...] = solved
    for peer in range(copies_ref.shape[0]):
        copies_ref[peer] = solved


def last_kernel(received_ref, right_ref, inverse_ref, *refs):
    earlier, out_ref = refs[:-1], refs[-1]
    for level, ref in enumerate(earlier):
        out_ref[level] = ref[...]
    out_ref[len(earlier)] = reduced_solve(received_ref, right_ref, inverse_ref)


def product_kernel(level, ids_ref, blocks_ref, *refs):
    gathered, out_ref = refs[:-1], refs[-1]
    slots = blocks_ref.shape[0]
    out_ref[...] = jnp.zeros_like(out_ref)
    count = ids_ref[3 * slots]
    products = []
    for s in range(slots):
        source_level = ids_ref[slots + s]
        position = ids_ref[2 * slots + s]
        operand = gathered[0][position]
        for other in range(1, level + 1):
            operand = jnp.where(source_level == other, gathered[other][position], operand)
        operand = jnp.where(s < count, operand, 0.0)
        products.append(mm_nt(operand, blocks_ref[s]))
    for s in range(slots):
        target = ids_ref[s]
        out_ref[target] = out_ref[target] + products[s]


def call(kernel, outs, in_spaces, flops, name):
    return pl.pallas_call(
        kernel,
        out_shape=outs,
        in_specs=[pl.BlockSpec(memory_space=space) for space in in_spaces],
        out_specs=jax.tree.map(lambda _: pl.BlockSpec(memory_space=VMEM), outs),
        cost_estimate=pl.CostEstimate(flops=flops, bytes_accessed=1 << 20, transcendentals=0),
        compiler_params=pltpu.CompilerParams(vmem_limit_bytes=16 << 20),
        name=name,
    )


def per_device(
    right_side, diag_blocks, off_blocks, slot_target, slot_level, slot_position, slot_count
):
    right_rows = right_side[:, 0, 0]
    diagonal = diag_blocks[:, 0, 0]
    blocks = off_blocks[0, 0]
    level_total, width_rhs, width = right_rows.shape
    row_peers = lax.axis_size("row")
    col_peers = lax.axis_size("col")
    f32 = jnp.float32
    solved_shape = jax.ShapeDtypeStruct((width_rhs, width), f32)
    copies_shape = jax.ShapeDtypeStruct((col_peers, width_rhs, width), f32)
    partial_shape = jax.ShapeDtypeStruct((row_peers, width_rhs, width), f32)
    out_shape = jax.ShapeDtypeStruct((level_total, width_rhs, width), f32)
    counts = jnp.broadcast_to(slot_count[0, 0][:, None], slot_target.shape[2:])
    ids = jnp.concatenate(
        [slot_target[0, 0], slot_level[0, 0], slot_position[0, 0], counts], axis=1
    )

    solved, copies = call(
        first_kernel, (solved_shape, copies_shape), (VMEM, VMEM), 1 << 26, "first"
    )(diagonal[0], right_rows[0])
    inverses = call(
        invert_kernel,
        jax.ShapeDtypeStruct((level_total - 1, width, width), f32),
        (VMEM,),
        1 << 28,
        "invert",
    )(diagonal[1:])
    results, gathered = [solved], []
    for level in range(level_total - 1):
        gathered.append(lax.all_to_all(copies, "col", 0, 0, tiled=True))
        partial = call(
            functools.partial(product_kernel, level),
            partial_shape,
            (SMEM,) + (VMEM,) * (level + 2),
            1 << 26,
            "products",
        )(ids[level], blocks[level], *gathered)
        received = lax.all_to_all(partial, "row", 0, 0, tiled=True)
        if level + 2 < level_total:
            solved, copies = call(
                solve_kernel, (solved_shape, copies_shape), (VMEM,) * 3, 1 << 24, "solve"
            )(received, right_rows[level + 1], inverses[level])
            results.append(solved)
        else:
            out = call(last_kernel, out_shape, (VMEM,) * (3 + len(results)), 1 << 24, "last")(
                received, right_rows[level + 1], inverses[level], *results
            )
    return out[:, None, None]


def solution(mesh):
    placed = (
        P(None, "row", "col", None, None),
        P(None, "row", "col", None, None),
        P("row", "col", None, None, None, None),
        P("row", "col", None, None),
        P("row", "col", None, None),
        P("row", "col", None, None),
        P("row", "col", None),
    )
    return jax.shard_map(
        per_device,
        mesh=mesh,
        in_specs=placed,
        out_specs=P(None, "row", "col", None, None),
        check_vma=False,
    )
```

```python
import functools

import jax
import jax.numpy as jnp
from jax import lax
from jax.experimental import pallas as pl
from jax.experimental.pallas import tpu as pltpu
from jax.sharding import Mesh
from jax.sharding import PartitionSpec as P

HIGHEST = lax.Precision.HIGHEST
VMEM = pltpu.VMEM
BASE = 32
GRANT = 16 << 20


def mm(a, b):
    return jnp.dot(a, b, precision=HIGHEST, preferred_element_type=jnp.float32)


def mm_nt(a, b):
    return lax.dot_general(
        a, b, (((1,), (1,)), ((), ())), precision=HIGHEST, preferred_element_type=jnp.float32
    )


def invert_lower(blocks):
    size = blocks[0].shape[0]
    rows = lax.broadcasted_iota(jnp.int32, (size, size), 0)
    cols = lax.broadcasted_iota(jnp.int32, (size, size), 1)
    eye = rows == cols
    strict = rows > cols
    same = (rows // BASE) == (cols // BASE)
    scaled, scale_cols, powers, inverses = [], [], [], []
    for block in blocks:
        on_diag = jnp.where(eye, block, 0.0)
        scale_rows = 1.0 / jnp.sum(on_diag, axis=1, keepdims=True)
        scale_cols.append(1.0 / jnp.sum(on_diag, axis=0, keepdims=True))
        m = jnp.where(strict, block * scale_rows, 0.0)
        scaled.append(m)
        local = jnp.where(same, m, 0.0)
        powers.append(local)
        inverses.append(jnp.where(eye, 1.0, 0.0) - local)
    span = 2
    while span < BASE:
        powers = [mm(p, p) for p in powers]
        inverses = [v + mm(v, p) for v, p in zip(inverses, powers)]
        span *= 2
    width = BASE
    while width < size:
        joins = ((rows // (2 * width)) == (cols // (2 * width))) & (
            (rows // width) > (cols // width)
        )
        steps = [mm(jnp.where(joins, m, 0.0), v) for m, v in zip(scaled, inverses)]
        inverses = [v - mm(v, s) for v, s in zip(inverses, steps)]
        width *= 2
    return [v * s for v, s in zip(inverses, scale_cols)]


def first_kernel(*refs):
    diag_hbm, right_hbm = refs[:2]
    inverse_ref, solved_ref, copies_ref = refs[7:10]
    kept_refs = refs[10:16]
    diag_ref, sems = refs[16:]
    moves = [pltpu.make_async_copy(diag_hbm, diag_ref, sems.at[0])]
    for at, (source, kept) in enumerate(zip(refs[1:7], kept_refs)):
        moves.append(pltpu.make_async_copy(source, kept, sems.at[at + 1]))
    for move in moves:
        move.start()
    moves[0].wait()
    moves[1].wait()
    level_total = diag_ref.shape[0]
    inverses = invert_lower([diag_ref[level, 0, 0] for level in range(level_total)])
    solved = mm_nt(kept_refs[0][0, 0, 0], inverses[0])
    solved_ref[...] = solved
    for peer in range(copies_ref.shape[0]):
        copies_ref[peer] = solved
    for level in range(1, level_total):
        inverse_ref[level - 1] = inverses[level]
    for move in moves[2:]:
        move.wait()


def reduced_solve(level, received_ref, right_ref, inverse_ref):
    total = received_ref[0]
    for peer in range(1, received_ref.shape[0]):
        total = total + received_ref[peer]
    return mm_nt(right_ref[level, 0, 0] - total, inverse_ref[level - 1])


def solve_kernel(level, received_ref, right_ref, inverse_ref, solved_ref, copies_ref):
    solved = reduced_solve(level, received_ref, right_ref, inverse_ref)
    solved_ref[...] = solved
    for peer in range(copies_ref.shape[0]):
        copies_ref[peer] = solved


def last_kernel(received_ref, right_ref, inverse_ref, *refs):
    earlier, out_ref = refs[:-1], refs[-1]
    for level, ref in enumerate(earlier):
        out_ref[level] = ref[...]
    level = len(earlier)
    out_ref[level] = reduced_solve(level, received_ref, right_ref, inverse_ref)


def split(value):
    high = value.astype(jnp.bfloat16)
    return high, (value - high.astype(jnp.float32)).astype(jnp.bfloat16)


def product(operand, block):
    rows = operand.shape[0]
    operand_high, operand_low = split(operand)
    block_high, block_low = split(block)
    contract = (((1,), (1,)), ((), ()))
    both = lax.dot_general(
        jnp.concatenate([operand_high, operand_low], axis=0),
        block_high,
        contract,
        preferred_element_type=jnp.float32,
    )
    rest = lax.dot_general(
        operand_high, block_low, contract, preferred_element_type=jnp.float32
    )
    return both[:rows] + (both[rows:] + rest)


def product_kernel(tier, target_ref, level_ref, position_ref, count_ref, blocks_ref, *refs):
    gathered, out_ref = refs[:-1], refs[-1]
    slots = blocks_ref.shape[3]
    out_ref[...] = jnp.zeros_like(out_ref)
    targets, source_levels = target_ref[0, 0, tier], level_ref[0, 0, tier]
    positions, count = position_ref[0, 0, tier], count_ref[0, 0][tier]
    products = []
    for s in range(slots):
        position = positions[s]
        near, far = position % 2, position // 2
        operand = gathered[0][near, far]
        for other in range(1, tier + 1):
            operand = jnp.where(source_levels[s] == other, gathered[other][near, far], operand)
        operand = jnp.where(s < count, operand, 0.0)
        products.append(product(operand, blocks_ref[0, 0, tier, s]))
    for s in range(slots):
        target = targets[s]
        out_ref[target] = out_ref[target] + products[s]


def call(kernel, outs, in_spaces, name, scratch=(), grant=16 << 20):
    return pl.pallas_call(
        kernel,
        out_shape=outs,
        in_specs=[pl.BlockSpec(memory_space=space) for space in in_spaces],
        out_specs=jax.tree.map(lambda _: pl.BlockSpec(memory_space=VMEM), outs),
        cost_estimate=pl.CostEstimate(flops=1 << 26, bytes_accessed=1 << 20, transcendentals=0),
        scratch_shapes=scratch,
        compiler_params=pltpu.CompilerParams(vmem_limit_bytes=grant),
        name=name,
    )


def collect(copies):
    strided = lax.all_to_all(copies, "far", 0, 0, tiled=True)
    return lax.all_gather(strided, "near", axis=0, tiled=False)


def per_device(
    right_side, diag_blocks, off_blocks, slot_target, slot_level, slot_position, slot_count
):
    level_total = right_side.shape[0]
    block = right_side.shape[3:]
    width = block[1]
    row_peers = lax.axis_size("chip") * lax.axis_size("core")
    f32 = jnp.float32
    solved_shape = jax.ShapeDtypeStruct(block, f32)
    copies_shape = jax.ShapeDtypeStruct((lax.axis_size("far"), *block), f32)
    partial_shape = jax.ShapeDtypeStruct((row_peers, *block), f32)
    out_shape = jax.ShapeDtypeStruct((level_total, *block), f32)
    inverse_shape = jax.ShapeDtypeStruct((level_total - 1, width, width), f32)

    kept = (right_side, off_blocks, slot_target, slot_level, slot_position, slot_count)
    kept_shapes = tuple(jax.ShapeDtypeStruct(array.shape, array.dtype) for array in kept)
    inverses, solved, copies, *kept = call(
        first_kernel,
        (inverse_shape, solved_shape, copies_shape, *kept_shapes),
        (pltpu.HBM,) * 7,
        "first",
        (pltpu.VMEM(diag_blocks.shape, f32), pltpu.SemaphoreType.DMA((7,))),
        GRANT,
    )(*(pltpu.with_memory_space_constraint(x, pltpu.HBM) for x in (diag_blocks, *kept)))
    right_side, off_blocks, *slot_tables = kept
    results, gathered = [solved], []
    for level in range(1, level_total):
        gathered.append(collect(copies))
        partial = call(
            functools.partial(product_kernel, level - 1),
            partial_shape,
            (VMEM,) * (level + 5),
            "products",
        )(*slot_tables, off_blocks, *gathered)
        received = lax.all_to_all(partial, ("chip", "core"), 0, 0, tiled=True)
        if level + 1 < level_total:
            solved, copies = call(
                functools.partial(solve_kernel, level),
                (solved_shape, copies_shape),
                (VMEM,) * 3,
                "solve",
            )(received, right_side, inverses)
            results.append(solved)
        else:
            out = call(last_kernel, out_shape, (VMEM,) * (3 + len(results)), "last")(
                received, right_side, inverses, *results
            )
    return out[:, None, None]


def solution(mesh):
    rows, cols = mesh.shape["row"], mesh.shape["col"]
    fine = Mesh(
        mesh.devices.reshape(rows // 2, 2, cols // 2, 2), ("chip", "core", "far", "near")
    )
    row, col = ("chip", "core"), ("far", "near")
    placed = (
        P(None, row, col, None, None),
        P(None, row, col, None, None),
        P(row, col, None, None, None, None),
        P(row, col, None, None),
        P(row, col, None, None),
        P(row, col, None, None),
        P(row, col, None),
    )
    return jax.shard_map(
        per_device,
        mesh=fine,
        in_specs=placed,
        out_specs=P(None, row, col, None, None),
        check_vma=False,
    )
```

```python
import functools

import jax
import jax.numpy as jnp
from jax import lax
from jax.experimental import pallas as pl
from jax.experimental.pallas import tpu as pltpu
from jax.sharding import Mesh
from jax.sharding import PartitionSpec as P

HIGHEST = lax.Precision.HIGHEST
VMEM = pltpu.VMEM
BASE = 32
GRANT = 16 << 20


def mm(a, b):
    return jnp.dot(a, b, precision=HIGHEST, preferred_element_type=jnp.float32)


def mm_nt(a, b):
    return lax.dot_general(
        a, b, (((1,), (1,)), ((), ())), precision=HIGHEST, preferred_element_type=jnp.float32
    )


def invert_lower(blocks):
    size = blocks[0].shape[0]
    rows = lax.broadcasted_iota(jnp.int32, (size, size), 0)
    cols = lax.broadcasted_iota(jnp.int32, (size, size), 1)
    eye = rows == cols
    strict = rows > cols
    same = (rows // BASE) == (cols // BASE)
    scaled, scale_cols, powers, inverses = [], [], [], []
    for block in blocks:
        on_diag = jnp.where(eye, block, 0.0)
        scale_rows = 1.0 / jnp.sum(on_diag, axis=1, keepdims=True)
        scale_cols.append(1.0 / jnp.sum(on_diag, axis=0, keepdims=True))
        m = jnp.where(strict, block * scale_rows, 0.0)
        scaled.append(m)
        local = jnp.where(same, m, 0.0)
        powers.append(local)
        inverses.append(jnp.where(eye, 1.0, 0.0) - local)
    span = 2
    while span < BASE:
        powers = [mm(p, p) for p in powers]
        inverses = [v + mm(v, p) for v, p in zip(inverses, powers)]
        span *= 2
    width = BASE
    while width < size:
        joins = ((rows // (2 * width)) == (cols // (2 * width))) & (
            (rows // width) > (cols // width)
        )
        steps = [mm(jnp.where(joins, m, 0.0), v) for m, v in zip(scaled, inverses)]
        inverses = [v - mm(v, s) for v, s in zip(inverses, steps)]
        width *= 2
    return [v * s for v, s in zip(inverses, scale_cols)]


def first_kernel(*refs):
    diag_hbm, right_hbm = refs[:2]
    inverse_ref, solved_ref, copies_ref = refs[7:10]
    kept_refs = refs[10:16]
    diag_ref, sems = refs[16:]
    moves = [pltpu.make_async_copy(diag_hbm, diag_ref, sems.at[0])]
    for at, (source, kept) in enumerate(zip(refs[1:7], kept_refs)):
        moves.append(pltpu.make_async_copy(source, kept, sems.at[at + 1]))
    for move in moves:
        move.start()
    moves[0].wait()
    moves[1].wait()
    level_total = diag_ref.shape[0]
    inverses = invert_lower([diag_ref[level, 0, 0] for level in range(level_total)])
    solved = mm_nt(kept_refs[0][0, 0, 0], inverses[0])
    solved_ref[...] = solved
    for peer in range(copies_ref.shape[0]):
        copies_ref[peer] = solved
    for level in range(1, level_total):
        inverse_ref[level - 1] = inverses[level]
    for move in moves[2:]:
        move.wait()


def reduced_solve(level, received_ref, right_ref, inverse_ref):
    total = received_ref[0]
    for peer in range(1, received_ref.shape[0]):
        total = total + received_ref[peer]
    return mm_nt(right_ref[level, 0, 0] - total, inverse_ref[level - 1])


def solve_kernel(level, received_ref, right_ref, inverse_ref, solved_ref, copies_ref):
    solved = reduced_solve(level, received_ref, right_ref, inverse_ref)
    solved_ref[...] = solved
    for peer in range(copies_ref.shape[0]):
        copies_ref[peer] = solved


def last_kernel(received_ref, right_ref, inverse_ref, *refs):
    earlier, out_ref = refs[:-1], refs[-1]
    for level, ref in enumerate(earlier):
        out_ref[level] = ref[...]
    level = len(earlier)
    out_ref[level] = reduced_solve(level, received_ref, right_ref, inverse_ref)


def split(value):
    high = value.astype(jnp.bfloat16)
    return high, (value - high.astype(jnp.float32)).astype(jnp.bfloat16)


def product(operand, block):
    rows = operand.shape[0]
    operand_high, operand_low = split(operand)
    block_high, block_low = split(block)
    contract = (((1,), (1,)), ((), ()))
    both = lax.dot_general(
        jnp.concatenate([operand_high, operand_low], axis=0),
        block_high,
        contract,
        preferred_element_type=jnp.float32,
    )
    rest = lax.dot_general(
        operand_high, block_low, contract, preferred_element_type=jnp.float32
    )
    return both[:rows] + (both[rows:] + rest)


def product_kernel(tier, target_ref, level_ref, position_ref, count_ref, blocks_ref, *refs):
    gathered, mine_ref, other_ref = refs[:-2], refs[-2], refs[-1]
    slots = blocks_ref.shape[3]
    mine_ref[...] = jnp.zeros_like(mine_ref)
    other_ref[...] = jnp.zeros_like(other_ref)
    me = lax.axis_index("core")
    targets, source_levels = target_ref[0, 0, tier], level_ref[0, 0, tier]
    positions, count = position_ref[0, 0, tier], count_ref[0, 0][tier]
    products = []
    for s in range(slots):
        position = positions[s]
        operand = gathered[0][position]
        for other in range(1, tier + 1):
            operand = jnp.where(source_levels[s] == other, gathered[other][position], operand)
        operand = jnp.where(s < count, operand, 0.0)
        products.append(product(operand, blocks_ref[0, 0, tier, s]))
    for s in range(slots):
        chip, is_mine = targets[s] // 2, targets[s] % 2 == me
        mine_ref[chip] = mine_ref[chip] + jnp.where(is_mine, products[s], 0.0)
        other_ref[chip] = other_ref[chip] + jnp.where(is_mine, 0.0, products[s])


def call(kernel, outs, in_spaces, name, scratch=(), grant=16 << 20):
    return pl.pallas_call(
        kernel,
        out_shape=outs,
        in_specs=[pl.BlockSpec(memory_space=space) for space in in_spaces],
        out_specs=jax.tree.map(lambda _: pl.BlockSpec(memory_space=VMEM), outs),
        cost_estimate=pl.CostEstimate(flops=1 << 26, bytes_accessed=1 << 20, transcendentals=0),
        scratch_shapes=scratch,
        compiler_params=pltpu.CompilerParams(vmem_limit_bytes=grant),
        name=name,
    )


def add_kernel(mine_ref, traded_ref, sum_ref):
    sum_ref[...] = mine_ref[...] + traded_ref[1 - lax.axis_index("core")]


def sum_at_owner(mine, other):
    traded = lax.all_gather(other, "core", axis=0, tiled=False)
    shape = jax.ShapeDtypeStruct(mine.shape, mine.dtype)
    both = call(add_kernel, shape, (VMEM, VMEM), "add")(mine, traded)
    return lax.all_to_all(both, "chip", 0, 0, tiled=True)


def per_device(
    right_side, diag_blocks, off_blocks, slot_target, slot_level, slot_position, slot_count
):
    level_total = right_side.shape[0]
    block = right_side.shape[3:]
    width = block[1]
    f32 = jnp.float32
    solved_shape = jax.ShapeDtypeStruct(block, f32)
    copies_shape = jax.ShapeDtypeStruct((lax.axis_size("col"), *block), f32)
    partial_shape = jax.ShapeDtypeStruct((lax.axis_size("chip"), *block), f32)
    out_shape = jax.ShapeDtypeStruct((level_total, *block), f32)
    inverse_shape = jax.ShapeDtypeStruct((level_total - 1, width, width), f32)

    kept = (right_side, off_blocks, slot_target, slot_level, slot_position, slot_count)
    kept_shapes = tuple(jax.ShapeDtypeStruct(array.shape, array.dtype) for array in kept)
    inverses, solved, copies, *kept = call(
        first_kernel,
        (inverse_shape, solved_shape, copies_shape, *kept_shapes),
        (pltpu.HBM,) * 7,
        "first",
        (pltpu.VMEM(diag_blocks.shape, f32), pltpu.SemaphoreType.DMA((7,))),
        GRANT,
    )(*(pltpu.with_memory_space_constraint(x, pltpu.HBM) for x in (diag_blocks, *kept)))
    right_side, off_blocks, *slot_tables = kept
    results, gathered = [solved], []
    for level in range(1, level_total):
        gathered.append(lax.all_to_all(copies, "col", 0, 0, tiled=True))
        mine, other = call(
            functools.partial(product_kernel, level - 1),
            (partial_shape, partial_shape),
            (VMEM,) * (level + 5),
            "products",
        )(*slot_tables, off_blocks, *gathered)
        received = sum_at_owner(mine, other)
        if level + 1 < level_total:
            solved, copies = call(
                functools.partial(solve_kernel, level),
                (solved_shape, copies_shape),
                (VMEM,) * 3,
                "solve",
            )(received, right_side, inverses)
            results.append(solved)
        else:
            out = call(last_kernel, out_shape, (VMEM,) * (3 + len(results)), "last")(
                received, right_side, inverses, *results
            )
    return out[:, None, None]


def solution(mesh):
    rows, cols = mesh.shape["row"], mesh.shape["col"]
    fine = Mesh(mesh.devices.reshape(rows // 2, 2, cols), ("chip", "core", "col"))
    row, col = ("chip", "core"), "col"
    placed = (
        P(None, row, col, None, None),
        P(None, row, col, None, None),
        P(row, col, None, None, None, None),
        P(row, col, None, None),
        P(row, col, None, None),
        P(row, col, None, None),
        P(row, col, None),
    )
    return jax.shard_map(
        per_device,
        mesh=fine,
        in_specs=placed,
        out_specs=P(None, row, col, None, None),
        check_vma=False,
    )
```

```python
import functools

import jax
import jax.numpy as jnp
from jax import lax
from jax.experimental import pallas as pl
from jax.experimental.pallas import tpu as pltpu
from jax.sharding import Mesh
from jax.sharding import PartitionSpec as P

HIGHEST = lax.Precision.HIGHEST
VMEM = pltpu.VMEM
BASE = 32
GRANT = 16 << 20


def mm(a, b):
    return jnp.dot(a, b, precision=HIGHEST, preferred_element_type=jnp.float32)


def mm_nt(a, b):
    return lax.dot_general(
        a, b, (((1,), (1,)), ((), ())), precision=HIGHEST, preferred_element_type=jnp.float32
    )


def invert_lower(blocks):
    size = blocks[0].shape[0]
    rows = lax.broadcasted_iota(jnp.int32, (size, size), 0)
    cols = lax.broadcasted_iota(jnp.int32, (size, size), 1)
    eye = rows == cols
    strict = rows > cols
    same = (rows // BASE) == (cols // BASE)
    scaled, scale_cols, powers, inverses = [], [], [], []
    for block in blocks:
        on_diag = jnp.where(eye, block, 0.0)
        scale_rows = 1.0 / jnp.sum(on_diag, axis=1, keepdims=True)
        scale_cols.append(1.0 / jnp.sum(on_diag, axis=0, keepdims=True))
        m = jnp.where(strict, block * scale_rows, 0.0)
        scaled.append(m)
        local = jnp.where(same, m, 0.0)
        powers.append(local)
        inverses.append(jnp.where(eye, 1.0, 0.0) - local)
    span = 2
    while span < BASE:
        powers = [mm(p, p) for p in powers]
        inverses = [v + mm(v, p) for v, p in zip(inverses, powers)]
        span *= 2
    width = BASE
    while width < size:
        joins = ((rows // (2 * width)) == (cols // (2 * width))) & (
            (rows // width) > (cols // width)
        )
        steps = [mm(jnp.where(joins, m, 0.0), v) for m, v in zip(scaled, inverses)]
        inverses = [v - mm(v, s) for v, s in zip(inverses, steps)]
        width *= 2
    return [v * s for v, s in zip(inverses, scale_cols)]


def first_kernel(*refs):
    diag_hbm, right_hbm, blocks_hbm = refs[:3]
    tables_hbm = refs[3:7]
    packed_ref, solved_ref, blocks_ref = refs[7:10]
    diag_ref, right_ref = refs[10:12]
    table_refs, sems = refs[12:16], refs[16]
    sources = (diag_hbm, right_hbm, *tables_hbm, blocks_hbm)
    targets = (diag_ref, right_ref, *table_refs, blocks_ref)
    moves = [
        pltpu.make_async_copy(source, target, sems.at[at])
        for at, (source, target) in enumerate(zip(sources, targets))
    ]
    for move in moves:
        move.start()
    moves[0].wait()
    moves[1].wait()
    level_total, width = diag_ref.shape[0], diag_ref.shape[-1]
    inverses = invert_lower([diag_ref[level, 0, 0] for level in range(level_total)])
    solved = mm_nt(right_ref[0, 0, 0], inverses[0])
    solved_ref[...] = solved
    at = Layout(level_total, *right_ref.shape[3:], table_refs[0].shape[2])
    packed_ref[at.solved : at.right] = solved
    for tier in range(level_total - 1):
        packed_ref[tier * width : (tier + 1) * width] = inverses[tier + 1]
        begin = at.right + tier * at.width_rhs
        packed_ref[begin : begin + at.width_rhs] = right_ref[tier + 1, 0, 0]
    packed_ref[at.tables : at.rows] = jnp.zeros((at.rows - at.tables, width), jnp.float32)
    for move in moves[2:-1]:
        move.wait()
    for table, ref in enumerate(table_refs[:3]):
        begin = at.tables + table * at.tiers
        packed_ref[begin : begin + at.tiers, : ref.shape[3]] = ref[0, 0].astype(jnp.float32)
    begin = at.tables + 3 * at.tiers
    packed_ref[begin : begin + 1, : at.tiers] = table_refs[3][0].astype(jnp.float32)
    moves[-1].wait()


class Layout:
    def __init__(self, level_total, width_rhs, width, tiers):
        self.width_rhs, self.width, self.tiers = width_rhs, width, tiers
        self.solved = (level_total - 1) * width
        self.right = self.solved + width_rhs
        self.tables = self.right + (level_total - 1) * width_rhs
        self.rows = self.tables + 4 * tiers

    def half(self, begin, me):
        size = self.width_rhs // 2
        return pl.ds(pl.multiple_of(begin + me * size, size), size)


def copy_to_all(copies_ref, row, value):
    for peer in range(copies_ref.shape[0]):
        copies_ref[peer, row] = value


def spread_kernel(at, both_ref, copies_ref):
    me = lax.axis_index("core")
    for row in range(2):
        copy_to_all(copies_ref, row, both_ref[row, at.half(at.solved, me)])


def reduced_solve(at, level, received_ref, both_ref):
    me = lax.axis_index("core")
    total = received_ref[0]
    for peer in range(1, received_ref.shape[0]):
        total = total + received_ref[peer]
    begin = at.right + (level - 1) * at.width_rhs
    inverse = pl.ds((level - 1) * at.width, at.width)
    return [
        mm_nt(both_ref[row, at.half(begin, me)] - total[row], both_ref[row, inverse])
        for row in range(2)
    ]


def solve_kernel(at, level, received_ref, both_ref, solved_ref, copies_ref):
    for row, solved in enumerate(reduced_solve(at, level, received_ref, both_ref)):
        solved_ref[row] = solved
        copy_to_all(copies_ref, row, solved)


def last_kernel(at, received_ref, both_ref, *refs):
    earlier, (mine_ref, other_ref, last_ref) = refs[:-3], refs[-3:]
    me = lax.axis_index("core")
    level = len(earlier) + 1
    for row, solved in enumerate(reduced_solve(at, level, received_ref, both_ref)):
        last_ref[row] = solved
    for tier, ref in enumerate((*earlier, last_ref)):
        mine_ref[tier] = ref[me]
        other_ref[tier] = ref[1 - me]


def join_kernel(solved_ref, mine_ref, traded_ref, out_ref):
    me = lax.axis_index("core")
    size = mine_ref.shape[1]
    out_ref[0] = solved_ref[...]
    for tier in range(mine_ref.shape[0]):
        out_ref[tier + 1, pl.ds(pl.multiple_of(me * size, size), size)] = mine_ref[tier]
        out_ref[tier + 1, pl.ds(pl.multiple_of((1 - me) * size, size), size)] = traded_ref[
            1 - me, tier
        ]


def split(value):
    high = value.astype(jnp.bfloat16)
    return high, (value - high.astype(jnp.float32)).astype(jnp.bfloat16)


def product(operand, block):
    rows = operand.shape[0]
    operand_high, operand_low = split(operand)
    block_high, block_low = split(block)
    contract = (((1,), (1,)), ((), ()))
    both = lax.dot_general(
        jnp.concatenate([operand_high, operand_low], axis=0),
        block_high,
        contract,
        preferred_element_type=jnp.float32,
    )
    rest = lax.dot_general(
        operand_high, block_low, contract, preferred_element_type=jnp.float32
    )
    return both[:rows] + (both[rows:] + rest)


def product_kernel(at, tier, both_ref, own_ref, other_ref, *refs):
    gathered, out_ref = refs[:-1], refs[-1]
    slots = own_ref.shape[3]
    out_ref[...] = jnp.zeros_like(out_ref)
    me = lax.axis_index("core")
    found = []
    for row, blocks_ref in ((me, own_ref), (1 - me, other_ref)):
        tables = [both_ref[row, at.tables + table * at.tiers + tier] for table in range(3)]
        targets, source_levels, positions = (table.astype(jnp.int32) for table in tables)
        counts = both_ref[row, at.tables + 3 * at.tiers].astype(jnp.int32)
        for s in range(slots):
            position = positions[s]
            operand = gathered[0][position, row]
            for other in range(1, tier + 1):
                operand = jnp.where(
                    source_levels[s] == other, gathered[other][position, row], operand
                )
            operand = jnp.where(s < counts[tier], operand, 0.0)
            found.append((targets[s], product(operand, blocks_ref[0, 0, tier, s])))
    for target, value in found:
        out_ref[target // 2, target % 2] = out_ref[target // 2, target % 2] + value


def call(kernel, outs, in_spaces, name, scratch=(), grant=16 << 20):
    return pl.pallas_call(
        kernel,
        out_shape=outs,
        in_specs=[pl.BlockSpec(memory_space=space) for space in in_spaces],
        out_specs=jax.tree.map(lambda _: pl.BlockSpec(memory_space=VMEM), outs),
        cost_estimate=pl.CostEstimate(flops=1 << 26, bytes_accessed=1 << 20, transcendentals=0),
        scratch_shapes=scratch,
        compiler_params=pltpu.CompilerParams(vmem_limit_bytes=grant),
        name=name,
    )


def per_device(
    right_side, diag_blocks, off_blocks, slot_target, slot_level, slot_position, slot_count
):
    level_total, _, _, width_rhs, width = right_side.shape
    tiers = level_total - 1
    at = Layout(level_total, width_rhs, width, tiers)
    half = (width_rhs // 2, width)

    def shape(*dims):
        return jax.ShapeDtypeStruct(dims, jnp.float32)

    solved_shape = shape(2, *half)
    copies_shape = shape(lax.axis_size("col"), 2, *half)
    partial_shape = shape(lax.axis_size("chip"), 2, *half)
    part_shape = shape(tiers, *half)
    inputs = (
        diag_blocks, right_side, off_blocks, slot_target, slot_level, slot_position, slot_count
    )

    packed, first_solved, own_blocks = call(
        first_kernel,
        (shape(at.rows, width), shape(width_rhs, width), shape(*off_blocks.shape)),
        (pltpu.HBM,) * 7,
        "first",
        (
            *(pltpu.VMEM(x.shape, x.dtype) for x in inputs[:2] + inputs[3:]),
            pltpu.SemaphoreType.DMA((7,)),
        ),
    )(*(pltpu.with_memory_space_constraint(x, pltpu.HBM) for x in inputs))
    other_blocks = lax.ppermute(off_blocks, "core", [(0, 1), (1, 0)])
    both = lax.all_gather(packed, "core", axis=0, tiled=False)
    copies = call(functools.partial(spread_kernel, at), copies_shape, (VMEM,), "spread")(both)
    results, gathered = [], []
    for level in range(1, level_total):
        gathered.append(lax.all_to_all(copies, "col", 0, 0, tiled=True))
        partial = call(
            functools.partial(product_kernel, at, level - 1),
            partial_shape,
            (VMEM,) * (3 + level),
            "products",
        )(both, own_blocks, other_blocks, *gathered)
        received = lax.all_to_all(partial, "chip", 0, 0, tiled=True)
        if level + 1 < level_total:
            solved, copies = call(
                functools.partial(solve_kernel, at, level),
                (solved_shape, copies_shape),
                (VMEM,) * 2,
                "solve",
            )(received, both)
            results.append(solved)
    mine, other, _ = call(
        functools.partial(last_kernel, at),
        (part_shape, part_shape, solved_shape),
        (VMEM,) * (2 + len(results)),
        "last",
    )(received, both, *results)
    traded = lax.all_gather(other, "core", axis=0, tiled=False)
    out = call(join_kernel, shape(level_total, width_rhs, width), (VMEM,) * 3, "join")(
        first_solved, mine, traded
    )
    return out[:, None, None]


def solution(mesh):
    rows, cols = mesh.shape["row"], mesh.shape["col"]
    fine = Mesh(mesh.devices.reshape(rows // 2, 2, cols), ("chip", "core", "col"))
    row, col = ("chip", "core"), "col"
    placed = (
        P(None, row, col, None, None),
        P(None, row, col, None, None),
        P(row, col, None, None, None, None),
        P(row, col, None, None),
        P(row, col, None, None),
        P(row, col, None, None),
        P(row, col, None),
    )
    return jax.shard_map(
        per_device,
        mesh=fine,
        in_specs=placed,
        out_specs=P(None, row, col, None, None),
        check_vma=False,
    )
```

```python
import functools

import jax
import jax.numpy as jnp
from jax import lax
from jax.experimental import pallas as pl
from jax.experimental.pallas import tpu as pltpu
from jax.sharding import Mesh
from jax.sharding import PartitionSpec as P

HIGHEST = lax.Precision.HIGHEST
VMEM = pltpu.VMEM
BASE = 32
GRANT = 16 << 20
HEAD_START = 2500


def mm(a, b):
    return jnp.dot(a, b, precision=HIGHEST, preferred_element_type=jnp.float32)


def mm_nt(a, b):
    return lax.dot_general(
        a, b, (((1,), (1,)), ((), ())), precision=HIGHEST, preferred_element_type=jnp.float32
    )


def invert_lower(blocks):
    size = blocks[0].shape[0]
    rows = lax.broadcasted_iota(jnp.int32, (size, size), 0)
    cols = lax.broadcasted_iota(jnp.int32, (size, size), 1)
    eye = rows == cols
    strict = rows > cols
    same = (rows // BASE) == (cols // BASE)
    scaled, scale_cols, powers, inverses = [], [], [], []
    for block in blocks:
        on_diag = jnp.where(eye, block, 0.0)
        scale_rows = 1.0 / jnp.sum(on_diag, axis=1, keepdims=True)
        scale_cols.append(1.0 / jnp.sum(on_diag, axis=0, keepdims=True))
        m = jnp.where(strict, block * scale_rows, 0.0)
        scaled.append(m)
        local = jnp.where(same, m, 0.0)
        powers.append(local)
        inverses.append(jnp.where(eye, 1.0, 0.0) - local)
    span = 2
    while span < BASE:
        powers = [mm(p, p) for p in powers]
        inverses = [v + mm(v, p) for v, p in zip(inverses, powers)]
        span *= 2
    width = BASE
    while width < size:
        joins = ((rows // (2 * width)) == (cols // (2 * width))) & (
            (rows // width) > (cols // width)
        )
        steps = [mm(jnp.where(joins, m, 0.0), v) for m, v in zip(scaled, inverses)]
        inverses = [v - mm(v, s) for v, s in zip(inverses, steps)]
        width *= 2
    return [v * s for v, s in zip(inverses, scale_cols)]


def first_kernel(*refs):
    diag_hbm, right_hbm, blocks_hbm = refs[:3]
    tables_hbm = refs[3:7]
    packed_ref, solved_ref, blocks_ref = refs[7:10]
    diag_ref, right_ref = refs[10:12]
    table_refs, sems = refs[12:16], refs[16]
    sources = (diag_hbm, right_hbm, *tables_hbm, blocks_hbm)
    targets = (diag_ref, right_ref, *table_refs, blocks_ref)
    moves = [
        pltpu.make_async_copy(source, target, sems.at[at])
        for at, (source, target) in enumerate(zip(sources, targets))
    ]
    for move in moves:
        move.start()
    moves[0].wait()
    moves[1].wait()
    level_total, width = diag_ref.shape[0], diag_ref.shape[-1]
    inverses = invert_lower([diag_ref[level, 0, 0] for level in range(level_total)])
    solved = mm_nt(right_ref[0, 0, 0], inverses[0])
    solved_ref[...] = solved
    at = Layout(level_total, *right_ref.shape[3:], table_refs[0].shape[2])
    packed_ref[at.solved : at.right] = solved
    for tier in range(level_total - 1):
        packed_ref[tier * width : (tier + 1) * width] = inverses[tier + 1]
        begin = at.right + tier * at.width_rhs
        packed_ref[begin : begin + at.width_rhs] = right_ref[tier + 1, 0, 0]
    packed_ref[at.tables : at.rows] = jnp.zeros((at.rows - at.tables, width), jnp.float32)
    for move in moves[2:-1]:
        move.wait()
    for table, ref in enumerate(table_refs[:3]):
        begin = at.tables + table * at.tiers
        packed_ref[begin : begin + at.tiers, : ref.shape[3]] = ref[0, 0].astype(jnp.float32)
    begin = at.tables + 3 * at.tiers
    packed_ref[begin : begin + 1, : at.tiers] = table_refs[3][0].astype(jnp.float32)
    moves[-1].wait()


class Layout:
    def __init__(self, level_total, width_rhs, width, tiers):
        self.width_rhs, self.width, self.tiers = width_rhs, width, tiers
        self.solved = (level_total - 1) * width
        self.right = self.solved + width_rhs
        self.tables = self.right + (level_total - 1) * width_rhs
        self.rows = self.tables + 4 * tiers

    def half(self, begin, me):
        size = self.width_rhs // 2
        return pl.ds(pl.multiple_of(begin + me * size, size), size)


def copy_to_all(copies_ref, row, value):
    for peer in range(copies_ref.shape[0]):
        copies_ref[peer, row] = value


def spread_kernel(at, both_ref, copies_ref, spent_ref):
    me = lax.axis_index("core")
    steps = jnp.where(me == 1, HEAD_START, 0)
    spent_ref[0] = lax.fori_loop(0, steps, lambda i, v: v * 5 + i, me)
    for row in range(2):
        copy_to_all(copies_ref, row, both_ref[row, at.half(at.solved, me)])


def reduced_solve(at, level, received_ref, both_ref):
    me = lax.axis_index("core")
    total = received_ref[0]
    for peer in range(1, received_ref.shape[0]):
        total = total + received_ref[peer]
    begin = at.right + (level - 1) * at.width_rhs
    inverse = pl.ds((level - 1) * at.width, at.width)
    return [
        mm_nt(both_ref[row, at.half(begin, me)] - total[row], both_ref[row, inverse])
        for row in range(2)
    ]


def solve_kernel(at, level, received_ref, both_ref, solved_ref, copies_ref):
    for row, solved in enumerate(reduced_solve(at, level, received_ref, both_ref)):
        solved_ref[row] = solved
        copy_to_all(copies_ref, row, solved)


def last_kernel(at, received_ref, both_ref, *refs):
    earlier, (mine_ref, other_ref, last_ref) = refs[:-3], refs[-3:]
    me = lax.axis_index("core")
    level = len(earlier) + 1
    for row, solved in enumerate(reduced_solve(at, level, received_ref, both_ref)):
        last_ref[row] = solved
    for tier, ref in enumerate((*earlier, last_ref)):
        mine_ref[tier] = ref[me]
        other_ref[tier] = ref[1 - me]


def join_kernel(solved_ref, mine_ref, traded_ref, out_ref):
    me = lax.axis_index("core")
    size = mine_ref.shape[1]
    out_ref[0] = solved_ref[...]
    for tier in range(mine_ref.shape[0]):
        out_ref[tier + 1, pl.ds(pl.multiple_of(me * size, size), size)] = mine_ref[tier]
        out_ref[tier + 1, pl.ds(pl.multiple_of((1 - me) * size, size), size)] = traded_ref[
            1 - me, tier
        ]


def split(value):
    high = value.astype(jnp.bfloat16)
    return high, (value - high.astype(jnp.float32)).astype(jnp.bfloat16)


def product(operand, block):
    rows = operand.shape[0]
    operand_high, operand_low = split(operand)
    block_high, block_low = split(block)
    contract = (((1,), (1,)), ((), ()))
    both = lax.dot_general(
        jnp.concatenate([operand_high, operand_low], axis=0),
        block_high,
        contract,
        preferred_element_type=jnp.float32,
    )
    rest = lax.dot_general(
        operand_high, block_low, contract, preferred_element_type=jnp.float32
    )
    return both[:rows] + (both[rows:] + rest)


def product_kernel(at, tier, both_ref, own_ref, other_ref, *refs):
    gathered, out_ref = refs[:-1], refs[-1]
    slots = own_ref.shape[3]
    out_ref[...] = jnp.zeros_like(out_ref)
    me = lax.axis_index("core")
    found = []
    for row, blocks_ref in ((me, own_ref), (1 - me, other_ref)):
        tables = [both_ref[row, at.tables + table * at.tiers + tier] for table in range(3)]
        targets, source_levels, positions = (table.astype(jnp.int32) for table in tables)
        counts = both_ref[row, at.tables + 3 * at.tiers].astype(jnp.int32)
        for s in range(slots):
            position = positions[s]
            operand = gathered[0][position, row]
            for other in range(1, tier + 1):
                operand = jnp.where(
                    source_levels[s] == other, gathered[other][position, row], operand
                )
            operand = jnp.where(s < counts[tier], operand, 0.0)
            found.append((targets[s], product(operand, blocks_ref[0, 0, tier, s])))
    for target, value in found:
        out_ref[target // 2, target % 2] = out_ref[target // 2, target % 2] + value


def call(kernel, outs, in_spaces, name, scratch=()):
    return pl.pallas_call(
        kernel,
        out_shape=outs,
        in_specs=[pl.BlockSpec(memory_space=space) for space in in_spaces],
        out_specs=jax.tree.map(lambda _: pl.BlockSpec(memory_space=VMEM), outs),
        cost_estimate=pl.CostEstimate(flops=1 << 26, bytes_accessed=1 << 20, transcendentals=0),
        scratch_shapes=scratch,
        compiler_params=pltpu.CompilerParams(vmem_limit_bytes=GRANT),
        name=name,
    )


def per_device(
    right_side, diag_blocks, off_blocks, slot_target, slot_level, slot_position, slot_count
):
    level_total, _, _, width_rhs, width = right_side.shape
    tiers = level_total - 1
    at = Layout(level_total, width_rhs, width, tiers)
    half = (width_rhs // 2, width)

    def shape(*dims):
        return jax.ShapeDtypeStruct(dims, jnp.float32)

    solved_shape = shape(2, *half)
    copies_shape = shape(lax.axis_size("col"), 2, *half)
    partial_shape = shape(lax.axis_size("chip"), 2, *half)
    part_shape = shape(tiers, *half)
    inputs = (
        diag_blocks, right_side, off_blocks, slot_target, slot_level, slot_position, slot_count
    )

    packed, first_solved, own_blocks = call(
        first_kernel,
        (shape(at.rows, width), shape(width_rhs, width), shape(*off_blocks.shape)),
        (pltpu.HBM,) * 7,
        "first",
        (
            *(pltpu.VMEM(x.shape, x.dtype) for x in inputs[:2] + inputs[3:]),
            pltpu.SemaphoreType.DMA((7,)),
        ),
    )(*(pltpu.with_memory_space_constraint(x, pltpu.HBM) for x in inputs))
    other_blocks = lax.ppermute(off_blocks, "core", [(0, 1), (1, 0)])
    both = lax.all_gather(packed, "core", axis=0, tiled=False)
    copies = call(
        functools.partial(spread_kernel, at),
        copies_shape,
        (VMEM,),
        "spread",
        (pltpu.SMEM((1,), jnp.int32),),
    )(both)
    results, gathered = [], []
    for level in range(1, level_total):
        gathered.append(lax.all_to_all(copies, "col", 0, 0, tiled=True))
        partial = call(
            functools.partial(product_kernel, at, level - 1),
            partial_shape,
            (VMEM,) * (3 + level),
            "products",
        )(both, own_blocks, other_blocks, *gathered)
        received = lax.all_to_all(partial, "chip", 0, 0, tiled=True)
        if level + 1 < level_total:
            solved, copies = call(
                functools.partial(solve_kernel, at, level),
                (solved_shape, copies_shape),
                (VMEM,) * 2,
                "solve",
            )(received, both)
            results.append(solved)
    mine, other = call(
        functools.partial(last_kernel, at),
        (part_shape, part_shape),
        (VMEM,) * (2 + len(results)),
        "last",
        (pltpu.VMEM((2, *half), jnp.float32),),
    )(received, both, *results)
    traded = lax.all_gather(other, "core", axis=0, tiled=False)
    out = call(join_kernel, shape(level_total, width_rhs, width), (VMEM,) * 3, "join")(
        first_solved, mine, traded
    )
    return out[:, None, None]


def solution(mesh):
    rows, cols = mesh.shape["row"], mesh.shape["col"]
    fine = Mesh(mesh.devices.reshape(rows // 2, 2, cols), ("chip", "core", "col"))
    row, col = ("chip", "core"), "col"
    placed = (
        P(None, row, col, None, None),
        P(None, row, col, None, None),
        P(row, col, None, None, None, None),
        P(row, col, None, None),
        P(row, col, None, None),
        P(row, col, None, None),
        P(row, col, None),
    )
    return jax.shard_map(
        per_device,
        mesh=fine,
        in_specs=placed,
        out_specs=P(None, row, col, None, None),
        check_vma=False,
    )
```

```python
import functools

import jax
import jax.numpy as jnp
from jax import lax
from jax.experimental import pallas as pl
from jax.experimental.pallas import tpu as pltpu
from jax.sharding import Mesh
from jax.sharding import PartitionSpec as P

HIGHEST = lax.Precision.HIGHEST
VMEM = pltpu.VMEM
BASE = 32
GRANT = 16 << 20
HEAD_START = 2400


def mm(a, b):
    return jnp.dot(a, b, precision=HIGHEST, preferred_element_type=jnp.float32)


def mm_nt(a, b):
    return lax.dot_general(
        a, b, (((1,), (1,)), ((), ())), precision=HIGHEST, preferred_element_type=jnp.float32
    )


def invert_lower(blocks):
    size = blocks[0].shape[0]
    rows = lax.broadcasted_iota(jnp.int32, (size, size), 0)
    cols = lax.broadcasted_iota(jnp.int32, (size, size), 1)
    eye = rows == cols
    strict = rows > cols
    same = (rows // BASE) == (cols // BASE)
    scaled, scale_cols, powers, inverses = [], [], [], []
    for block in blocks:
        on_diag = jnp.where(eye, block, 0.0)
        scale_rows = 1.0 / jnp.sum(on_diag, axis=1, keepdims=True)
        scale_cols.append(1.0 / jnp.sum(on_diag, axis=0, keepdims=True))
        m = jnp.where(strict, block * scale_rows, 0.0)
        scaled.append(m)
        local = jnp.where(same, m, 0.0)
        powers.append(local)
        inverses.append(jnp.where(eye, 1.0, 0.0) - local)
    span = 2
    while span < BASE:
        powers = [mm(p, p) for p in powers]
        inverses = [v + mm(v, p) for v, p in zip(inverses, powers)]
        span *= 2
    width = BASE
    while width < size:
        joins = ((rows // (2 * width)) == (cols // (2 * width))) & (
            (rows // width) > (cols // width)
        )
        steps = [mm(jnp.where(joins, m, 0.0), v) for m, v in zip(scaled, inverses)]
        inverses = [v - mm(v, s) for v, s in zip(inverses, steps)]
        width *= 2
    return [v * s for v, s in zip(inverses, scale_cols)]


def first_kernel(*refs):
    diag_hbm, right_hbm, blocks_hbm = refs[:3]
    tables_hbm = refs[3:7]
    packed_ref, solved_ref, blocks_ref = refs[7:10]
    diag_ref, right_ref = refs[10:12]
    table_refs, sems = refs[12:16], refs[16]
    sources = (diag_hbm, right_hbm, *tables_hbm, blocks_hbm)
    targets = (diag_ref, right_ref, *table_refs, blocks_ref)
    moves = [
        pltpu.make_async_copy(source, target, sems.at[at])
        for at, (source, target) in enumerate(zip(sources, targets))
    ]
    for move in moves:
        move.start()
    moves[0].wait()
    moves[1].wait()
    level_total, width = diag_ref.shape[0], diag_ref.shape[-1]
    inverses = invert_lower([diag_ref[level, 0, 0] for level in range(level_total)])
    solved = mm_nt(right_ref[0, 0, 0], inverses[0])
    solved_ref[...] = solved
    at = Layout(level_total, *right_ref.shape[3:], table_refs[0].shape[2])
    packed_ref[at.solved : at.right] = solved
    for tier in range(level_total - 1):
        packed_ref[tier * width : (tier + 1) * width] = inverses[tier + 1]
        begin = at.right + tier * at.width_rhs
        packed_ref[begin : begin + at.width_rhs] = right_ref[tier + 1, 0, 0]
    packed_ref[at.tables : at.rows] = jnp.zeros((at.rows - at.tables, width), jnp.float32)
    for move in moves[2:-1]:
        move.wait()
    for table, ref in enumerate(table_refs[:3]):
        begin = at.tables + table * at.tiers
        packed_ref[begin : begin + at.tiers, : ref.shape[3]] = ref[0, 0].astype(jnp.float32)
    begin = at.tables + 3 * at.tiers
    packed_ref[begin : begin + 1, : at.tiers] = table_refs[3][0].astype(jnp.float32)
    moves[-1].wait()


class Layout:
    def __init__(self, level_total, width_rhs, width, tiers):
        self.width_rhs, self.width, self.tiers = width_rhs, width, tiers
        self.solved = (level_total - 1) * width
        self.right = self.solved + width_rhs
        self.tables = self.right + (level_total - 1) * width_rhs
        self.rows = self.tables + 4 * tiers

    def half(self, begin, me):
        size = self.width_rhs // 2
        return pl.ds(pl.multiple_of(begin + me * size, size), size)


def copy_to_all(copies_ref, row, value):
    for peer in range(copies_ref.shape[0]):
        copies_ref[peer, row] = value


def spread_kernel(at, both_ref, copies_ref, spent_ref):
    me = lax.axis_index("core")
    steps = jnp.where(me == 1, HEAD_START, 0)
    spent_ref[0] = lax.fori_loop(0, steps, lambda i, v: v * 5 + i, me)
    for row in range(2):
        copy_to_all(copies_ref, row, both_ref[row, at.half(at.solved, me)])


def reduced_solve(at, level, received_ref, both_ref):
    me = lax.axis_index("core")
    total = received_ref[0]
    for peer in range(1, received_ref.shape[0]):
        total = total + received_ref[peer]
    begin = at.right + (level - 1) * at.width_rhs
    inverse = pl.ds((level - 1) * at.width, at.width)
    return [
        mm_nt(both_ref[row, at.half(begin, me)] - total[row], both_ref[row, inverse])
        for row in range(2)
    ]


def solve_kernel(at, level, received_ref, both_ref, solved_ref, copies_ref):
    for row, solved in enumerate(reduced_solve(at, level, received_ref, both_ref)):
        solved_ref[row] = solved
        copy_to_all(copies_ref, row, solved)


def last_kernel(at, received_ref, both_ref, *refs):
    earlier, (mine_ref, other_ref, last_ref) = refs[:-3], refs[-3:]
    me = lax.axis_index("core")
    level = len(earlier) + 1
    for row, solved in enumerate(reduced_solve(at, level, received_ref, both_ref)):
        last_ref[row] = solved
    for tier, ref in enumerate((*earlier, last_ref)):
        mine_ref[tier] = ref[me]
        other_ref[tier] = ref[1 - me]


def join_kernel(solved_ref, mine_ref, traded_ref, out_ref):
    me = lax.axis_index("core")
    size = mine_ref.shape[1]
    out_ref[0] = solved_ref[...]
    for tier in range(mine_ref.shape[0]):
        out_ref[tier + 1, pl.ds(pl.multiple_of(me * size, size), size)] = mine_ref[tier]
        out_ref[tier + 1, pl.ds(pl.multiple_of((1 - me) * size, size), size)] = traded_ref[
            1 - me, tier
        ]


def split(value):
    high = value.astype(jnp.bfloat16)
    return high, (value - high.astype(jnp.float32)).astype(jnp.bfloat16)


def product(operand, block):
    rows, columns = operand.shape[0], block.shape[0]
    parts = lax.dot_general(
        jnp.concatenate(split(operand), axis=0),
        jnp.concatenate(split(block), axis=0),
        (((1,), (1,)), ((), ())),
        preferred_element_type=jnp.float32,
    )
    smaller = parts[rows:, :columns] + (parts[:rows, columns:] + parts[rows:, columns:])
    return parts[:rows, :columns] + smaller


def product_kernel(at, tier, both_ref, own_ref, other_ref, *refs):
    gathered, out_ref = refs[:-1], refs[-1]
    slots = own_ref.shape[3]
    out_ref[...] = jnp.zeros_like(out_ref)
    me = lax.axis_index("core")
    found = []
    for row, blocks_ref in ((me, own_ref), (1 - me, other_ref)):
        tables = [both_ref[row, at.tables + table * at.tiers + tier] for table in range(3)]
        targets, source_levels, positions = (table.astype(jnp.int32) for table in tables)
        counts = both_ref[row, at.tables + 3 * at.tiers].astype(jnp.int32)
        for s in range(slots):
            position = positions[s]
            operand = gathered[0][position, row]
            for other in range(1, tier + 1):
                operand = jnp.where(
                    source_levels[s] == other, gathered[other][position, row], operand
                )
            operand = jnp.where(s < counts[tier], operand, 0.0)
            found.append((targets[s], product(operand, blocks_ref[0, 0, tier, s])))
    for target, value in found:
        out_ref[target // 2, target % 2] = out_ref[target // 2, target % 2] + value


def call(kernel, outs, in_spaces, name, scratch=()):
    return pl.pallas_call(
        kernel,
        out_shape=outs,
        in_specs=[pl.BlockSpec(memory_space=space) for space in in_spaces],
        out_specs=jax.tree.map(lambda _: pl.BlockSpec(memory_space=VMEM), outs),
        cost_estimate=pl.CostEstimate(flops=1 << 26, bytes_accessed=1 << 20, transcendentals=0),
        scratch_shapes=scratch,
        compiler_params=pltpu.CompilerParams(vmem_limit_bytes=GRANT),
        name=name,
    )


def per_device(
    right_side, diag_blocks, off_blocks, slot_target, slot_level, slot_position, slot_count
):
    level_total, _, _, width_rhs, width = right_side.shape
    tiers = level_total - 1
    at = Layout(level_total, width_rhs, width, tiers)
    half = (width_rhs // 2, width)

    def shape(*dims):
        return jax.ShapeDtypeStruct(dims, jnp.float32)

    solved_shape = shape(2, *half)
    copies_shape = shape(lax.axis_size("col"), 2, *half)
    partial_shape = shape(lax.axis_size("chip"), 2, *half)
    part_shape = shape(tiers, *half)
    inputs = (
        diag_blocks, right_side, off_blocks, slot_target, slot_level, slot_position, slot_count
    )

    packed, first_solved, own_blocks = call(
        first_kernel,
        (shape(at.rows, width), shape(width_rhs, width), shape(*off_blocks.shape)),
        (pltpu.HBM,) * 7,
        "first",
        (
            *(pltpu.VMEM(x.shape, x.dtype) for x in inputs[:2] + inputs[3:]),
            pltpu.SemaphoreType.DMA((7,)),
        ),
    )(*(pltpu.with_memory_space_constraint(x, pltpu.HBM) for x in inputs))
    other_blocks = lax.ppermute(off_blocks, "core", [(0, 1), (1, 0)])
    both = lax.all_gather(packed, "core", axis=0, tiled=False)
    copies = call(
        functools.partial(spread_kernel, at),
        copies_shape,
        (VMEM,),
        "spread",
        (pltpu.SMEM((1,), jnp.int32),),
    )(both)
    results, gathered = [], []
    for level in range(1, level_total):
        gathered.append(lax.all_to_all(copies, "col", 0, 0, tiled=True))
        partial = call(
            functools.partial(product_kernel, at, level - 1),
            partial_shape,
            (VMEM,) * (3 + level),
            "products",
        )(both, own_blocks, other_blocks, *gathered)
        received = lax.all_to_all(partial, "chip", 0, 0, tiled=True)
        if level + 1 < level_total:
            solved, copies = call(
                functools.partial(solve_kernel, at, level),
                (solved_shape, copies_shape),
                (VMEM,) * 2,
                "solve",
            )(received, both)
            results.append(solved)
    mine, other = call(
        functools.partial(last_kernel, at),
        (part_shape, part_shape),
        (VMEM,) * (2 + len(results)),
        "last",
        (pltpu.VMEM((2, *half), jnp.float32),),
    )(received, both, *results)
    traded = lax.all_gather(other, "core", axis=0, tiled=False)
    out = call(join_kernel, shape(level_total, width_rhs, width), (VMEM,) * 3, "join")(
        first_solved, mine, traded
    )
    return out[:, None, None]


def solution(mesh):
    rows, cols = mesh.shape["row"], mesh.shape["col"]
    fine = Mesh(mesh.devices.reshape(rows // 2, 2, cols), ("chip", "core", "col"))
    row, col = ("chip", "core"), "col"
    placed = (
        P(None, row, col, None, None),
        P(None, row, col, None, None),
        P(row, col, None, None, None, None),
        P(row, col, None, None),
        P(row, col, None, None),
        P(row, col, None, None),
        P(row, col, None),
    )
    return jax.shard_map(
        per_device,
        mesh=fine,
        in_specs=placed,
        out_specs=P(None, row, col, None, None),
        check_vma=False,
    )
```

```python
import functools

import jax
import jax.numpy as jnp
from jax import lax
from jax.experimental import pallas as pl
from jax.experimental.pallas import tpu as pltpu
from jax.sharding import Mesh
from jax.sharding import PartitionSpec as P

HIGHEST = lax.Precision.HIGHEST
VMEM = pltpu.VMEM
BASE = 32
GRANT = 16 << 20
HEAD_START = 2400


def mm(a, b):
    return jnp.dot(a, b, precision=HIGHEST, preferred_element_type=jnp.float32)


def mm_nt(a, b):
    return lax.dot_general(
        a, b, (((1,), (1,)), ((), ())), precision=HIGHEST, preferred_element_type=jnp.float32
    )


def invert_lower(blocks):
    size = blocks[0].shape[0]
    rows = lax.broadcasted_iota(jnp.int32, (size, size), 0)
    cols = lax.broadcasted_iota(jnp.int32, (size, size), 1)
    eye = rows == cols
    strict = rows > cols
    same = (rows // BASE) == (cols // BASE)
    scaled, scale_cols, powers, inverses = [], [], [], []
    for block in blocks:
        on_diag = jnp.where(eye, block, 0.0)
        scale_rows = 1.0 / jnp.sum(on_diag, axis=1, keepdims=True)
        scale_cols.append(1.0 / jnp.sum(on_diag, axis=0, keepdims=True))
        m = jnp.where(strict, block * scale_rows, 0.0)
        scaled.append(m)
        local = jnp.where(same, m, 0.0)
        powers.append(local)
        inverses.append(jnp.where(eye, 1.0, 0.0) - local)
    span = 2
    while span < BASE:
        powers = [mm(p, p) for p in powers]
        inverses = [v + mm(v, p) for v, p in zip(inverses, powers)]
        span *= 2
    width = BASE
    while 2 * width < size:
        joins = ((rows // (2 * width)) == (cols // (2 * width))) & (
            (rows // width) > (cols // width)
        )
        steps = [mm(jnp.where(joins, m, 0.0), v) for m, v in zip(scaled, inverses)]
        inverses = [v - mm(v, s) for v, s in zip(inverses, steps)]
        width *= 2
    left = cols[width:] < width
    steps = [mm(jnp.where(left, m[width:], 0.0), v) for m, v in zip(scaled, inverses)]
    steps = [jnp.concatenate([jnp.zeros_like(t), t], axis=0) for t in steps]
    inverses = [
        jnp.concatenate([v[:width], v[width:] - mm(v[width:], t)], axis=0)
        for v, t in zip(inverses, steps)
    ]
    return [v * s for v, s in zip(inverses, scale_cols)]


def first_kernel(*refs):
    diag_hbm, right_hbm, blocks_hbm = refs[:3]
    tables_hbm = refs[3:7]
    packed_ref, solved_ref, blocks_ref = refs[7:10]
    diag_ref, right_ref = refs[10:12]
    table_refs, sems = refs[12:16], refs[16]
    sources = (diag_hbm, right_hbm, *tables_hbm, blocks_hbm)
    targets = (diag_ref, right_ref, *table_refs, blocks_ref)
    moves = [
        pltpu.make_async_copy(source, target, sems.at[at])
        for at, (source, target) in enumerate(zip(sources, targets))
    ]
    for move in moves:
        move.start()
    moves[0].wait()
    moves[1].wait()
    level_total, width = diag_ref.shape[0], diag_ref.shape[-1]
    inverses = invert_lower([diag_ref[level, 0, 0] for level in range(level_total)])
    solved = mm_nt(right_ref[0, 0, 0], inverses[0])
    solved_ref[...] = solved
    at = Layout(level_total, *right_ref.shape[3:], table_refs[0].shape[2])
    packed_ref[at.solved : at.right] = solved
    for tier in range(level_total - 1):
        packed_ref[tier * width : (tier + 1) * width] = inverses[tier + 1]
        begin = at.right + tier * at.width_rhs
        packed_ref[begin : begin + at.width_rhs] = right_ref[tier + 1, 0, 0]
    packed_ref[at.tables : at.rows] = jnp.zeros((at.rows - at.tables, width), jnp.float32)
    for move in moves[2:-1]:
        move.wait()
    for table, ref in enumerate(table_refs[:3]):
        begin = at.tables + table * at.tiers
        packed_ref[begin : begin + at.tiers, : ref.shape[3]] = ref[0, 0].astype(jnp.float32)
    begin = at.tables + 3 * at.tiers
    packed_ref[begin : begin + 1, : at.tiers] = table_refs[3][0].astype(jnp.float32)
    moves[-1].wait()


class Layout:
    def __init__(self, level_total, width_rhs, width, tiers):
        self.width_rhs, self.width, self.tiers = width_rhs, width, tiers
        self.solved = (level_total - 1) * width
        self.right = self.solved + width_rhs
        self.tables = self.right + (level_total - 1) * width_rhs
        self.rows = self.tables + 4 * tiers

    def half(self, begin, me):
        size = self.width_rhs // 2
        return pl.ds(pl.multiple_of(begin + me * size, size), size)


def copy_to_all(copies_ref, row, value):
    for peer in range(copies_ref.shape[0]):
        copies_ref[peer, row] = value


def spread_kernel(at, both_ref, copies_ref, spent_ref):
    me = lax.axis_index("core")
    steps = jnp.where(me == 1, HEAD_START, 0)
    spent_ref[0] = lax.fori_loop(0, steps, lambda i, v: v * 5 + i, me)
    for row in range(2):
        copy_to_all(copies_ref, row, both_ref[row, at.half(at.solved, me)])


def reduced_solve(at, level, received_ref, both_ref):
    me = lax.axis_index("core")
    total = received_ref[0]
    for peer in range(1, received_ref.shape[0]):
        total = total + received_ref[peer]
    begin = at.right + (level - 1) * at.width_rhs
    inverse = pl.ds((level - 1) * at.width, at.width)
    return [
        mm_nt(both_ref[row, at.half(begin, me)] - total[row], both_ref[row, inverse])
        for row in range(2)
    ]


def solve_kernel(at, level, received_ref, both_ref, solved_ref, copies_ref):
    for row, solved in enumerate(reduced_solve(at, level, received_ref, both_ref)):
        solved_ref[row] = solved
        copy_to_all(copies_ref, row, solved)


def last_kernel(at, received_ref, both_ref, *refs):
    earlier, (mine_ref, other_ref, last_ref) = refs[:-3], refs[-3:]
    me = lax.axis_index("core")
    level = len(earlier) + 1
    for row, solved in enumerate(reduced_solve(at, level, received_ref, both_ref)):
        last_ref[row] = solved
    for tier, ref in enumerate((*earlier, last_ref)):
        mine_ref[tier] = ref[me]
        other_ref[tier] = ref[1 - me]


def join_kernel(solved_ref, mine_ref, traded_ref, out_ref, sems):
    me = lax.axis_index("core")
    tiers, size = mine_ref.shape[:2]

    def half_of(core):
        return out_ref.at[pl.ds(1, tiers), pl.ds(pl.multiple_of(core * size, size), size)]

    moves = [
        pltpu.make_async_copy(solved_ref, out_ref.at[0], sems.at[0]),
        pltpu.make_async_copy(mine_ref, half_of(me), sems.at[1]),
        pltpu.make_async_copy(traded_ref.at[1 - me], half_of(1 - me), sems.at[2]),
    ]
    for move in moves:
        move.start()
    for move in moves:
        move.wait()


def split(value):
    high = value.astype(jnp.bfloat16)
    return high, (value - high.astype(jnp.float32)).astype(jnp.bfloat16)


def product(operand, block):
    rows, columns = operand.shape[0], block.shape[0]
    parts = lax.dot_general(
        jnp.concatenate(split(operand), axis=0),
        jnp.concatenate(split(block), axis=0),
        (((1,), (1,)), ((), ())),
        preferred_element_type=jnp.float32,
    )
    smaller = parts[rows:, :columns] + (parts[:rows, columns:] + parts[rows:, columns:])
    return parts[:rows, :columns] + smaller


def product_kernel(at, tier, both_ref, own_ref, other_ref, *refs):
    gathered, out_ref = refs[:-1], refs[-1]
    slots = own_ref.shape[3]
    out_ref[...] = jnp.zeros_like(out_ref)
    me = lax.axis_index("core")
    found = []
    for row, blocks_ref in ((me, own_ref), (1 - me, other_ref)):
        tables = [both_ref[row, at.tables + table * at.tiers + tier] for table in range(3)]
        targets, source_levels, positions = (table.astype(jnp.int32) for table in tables)
        counts = both_ref[row, at.tables + 3 * at.tiers].astype(jnp.int32)
        for s in range(slots):
            position = positions[s]
            operand = gathered[0][position, row]
            for other in range(1, tier + 1):
                operand = jnp.where(
                    source_levels[s] == other, gathered[other][position, row], operand
                )
            operand = jnp.where(s < counts[tier], operand, 0.0)
            found.append((targets[s], product(operand, blocks_ref[0, 0, tier, s])))
    for target, value in found:
        out_ref[target // 2, target % 2] = out_ref[target // 2, target % 2] + value


def call(kernel, outs, in_spaces, name, scratch=()):
    return pl.pallas_call(
        kernel,
        out_shape=outs,
        in_specs=[pl.BlockSpec(memory_space=space) for space in in_spaces],
        out_specs=jax.tree.map(lambda _: pl.BlockSpec(memory_space=VMEM), outs),
        cost_estimate=pl.CostEstimate(flops=1 << 26, bytes_accessed=1 << 20, transcendentals=0),
        scratch_shapes=scratch,
        compiler_params=pltpu.CompilerParams(vmem_limit_bytes=GRANT),
        name=name,
    )


def per_device(
    right_side, diag_blocks, off_blocks, slot_target, slot_level, slot_position, slot_count
):
    level_total, _, _, width_rhs, width = right_side.shape
    tiers = level_total - 1
    at = Layout(level_total, width_rhs, width, tiers)
    half = (width_rhs // 2, width)

    def shape(*dims):
        return jax.ShapeDtypeStruct(dims, jnp.float32)

    solved_shape = shape(2, *half)
    copies_shape = shape(lax.axis_size("col"), 2, *half)
    partial_shape = shape(lax.axis_size("chip"), 2, *half)
    part_shape = shape(tiers, *half)
    inputs = (
        diag_blocks, right_side, off_blocks, slot_target, slot_level, slot_position, slot_count
    )

    packed, first_solved, own_blocks = call(
        first_kernel,
        (shape(at.rows, width), shape(width_rhs, width), shape(*off_blocks.shape)),
        (pltpu.HBM,) * 7,
        "first",
        (
            *(pltpu.VMEM(x.shape, x.dtype) for x in inputs[:2] + inputs[3:]),
            pltpu.SemaphoreType.DMA((7,)),
        ),
    )(*(pltpu.with_memory_space_constraint(x, pltpu.HBM) for x in inputs))
    other_blocks = lax.ppermute(off_blocks, "core", [(0, 1), (1, 0)])
    both = lax.all_gather(packed, "core", axis=0, tiled=False)
    copies = call(
        functools.partial(spread_kernel, at),
        copies_shape,
        (VMEM,),
        "spread",
        (pltpu.SMEM((1,), jnp.int32),),
    )(both)
    results, gathered = [], []
    for level in range(1, level_total):
        gathered.append(lax.all_to_all(copies, "col", 0, 0, tiled=True))
        partial = call(
            functools.partial(product_kernel, at, level - 1),
            partial_shape,
            (VMEM,) * (3 + level),
            "products",
        )(both, own_blocks, other_blocks, *gathered)
        received = lax.all_to_all(partial, "chip", 0, 0, tiled=True)
        if level + 1 < level_total:
            solved, copies = call(
                functools.partial(solve_kernel, at, level),
                (solved_shape, copies_shape),
                (VMEM,) * 2,
                "solve",
            )(received, both)
            results.append(solved)
    mine, other = call(
        functools.partial(last_kernel, at),
        (part_shape, part_shape),
        (VMEM,) * (2 + len(results)),
        "last",
        (pltpu.VMEM((2, *half), jnp.float32),),
    )(received, both, *results)
    traded = lax.all_gather(other, "core", axis=0, tiled=False)
    out = pl.pallas_call(
        join_kernel,
        out_shape=shape(level_total, width_rhs, width),
        in_specs=[pl.BlockSpec(memory_space=VMEM)] * 3,
        out_specs=pl.BlockSpec(memory_space=pltpu.HBM),
        scratch_shapes=(pltpu.SemaphoreType.DMA((3,)),),
        compiler_params=pltpu.CompilerParams(vmem_limit_bytes=GRANT),
        name="join",
    )(first_solved, mine, traded)
    return out[:, None, None]


def solution(mesh):
    rows, cols = mesh.shape["row"], mesh.shape["col"]
    fine = Mesh(mesh.devices.reshape(rows // 2, 2, cols), ("chip", "core", "col"))
    row, col = ("chip", "core"), "col"
    placed = (
        P(None, row, col, None, None),
        P(None, row, col, None, None),
        P(row, col, None, None, None, None),
        P(row, col, None, None),
        P(row, col, None, None),
        P(row, col, None, None),
        P(row, col, None),
    )
    return jax.shard_map(
        per_device,
        mesh=fine,
        in_specs=placed,
        out_specs=P(None, row, col, None, None),
        check_vma=False,
    )
```

```python
import functools

import jax
import jax.numpy as jnp
from jax import lax
from jax.experimental import pallas as pl
from jax.experimental.pallas import tpu as pltpu
from jax.sharding import Mesh
from jax.sharding import PartitionSpec as P

HIGHEST = lax.Precision.HIGHEST
VMEM = pltpu.VMEM
BASE = 32
GRANT = 16 << 20
HEAD_START = 2350


def mm(a, b):
    return jnp.dot(a, b, precision=HIGHEST, preferred_element_type=jnp.float32)


def mm_nt(a, b):
    return lax.dot_general(
        a, b, (((1,), (1,)), ((), ())), precision=HIGHEST, preferred_element_type=jnp.float32
    )


def invert_lower(blocks):
    size = blocks[0].shape[0]
    rows = lax.broadcasted_iota(jnp.int32, (size, size), 0)
    cols = lax.broadcasted_iota(jnp.int32, (size, size), 1)
    eye = rows == cols
    strict = rows > cols
    same = (rows // BASE) == (cols // BASE)
    scaled, scale_cols, powers, inverses = [], [], [], []
    for block in blocks:
        on_diag = jnp.where(eye, block, 0.0)
        scale_rows = 1.0 / jnp.sum(on_diag, axis=1, keepdims=True)
        scale_cols.append(1.0 / jnp.sum(on_diag, axis=0, keepdims=True))
        m = jnp.where(strict, block * scale_rows, 0.0)
        scaled.append(m)
        local = jnp.where(same, m, 0.0)
        powers.append(local)
        inverses.append(jnp.where(eye, 1.0, 0.0) - local)
    span = 2
    while span < BASE:
        powers = [mm(p, p) for p in powers]
        inverses = [v + mm(v, p) for v, p in zip(inverses, powers)]
        span *= 2
    width = BASE
    while 2 * width < size:
        joins = ((rows // (2 * width)) == (cols // (2 * width))) & (
            (rows // width) > (cols // width)
        )
        steps = [mm(jnp.where(joins, m, 0.0), v) for m, v in zip(scaled, inverses)]
        inverses = [v - mm(v, s) for v, s in zip(inverses, steps)]
        width *= 2
    left = cols[width:] < width
    steps = [mm(jnp.where(left, m[width:], 0.0), v) for m, v in zip(scaled, inverses)]
    steps = [jnp.concatenate([jnp.zeros_like(t), t], axis=0) for t in steps]
    inverses = [
        jnp.concatenate([v[:width], v[width:] - mm(v[width:], t)], axis=0)
        for v, t in zip(inverses, steps)
    ]
    return [v * s for v, s in zip(inverses, scale_cols)]


def first_kernel(*refs):
    diag_hbm, right_hbm, blocks_hbm = refs[:3]
    tables_hbm = refs[3:7]
    packed_ref, solved_ref, blocks_ref = refs[7:10]
    diag_ref, right_ref = refs[10:12]
    table_refs, sems = refs[12:16], refs[16]
    sources = (diag_hbm, right_hbm, *tables_hbm, blocks_hbm)
    targets = (diag_ref, right_ref, *table_refs, blocks_ref)
    moves = [
        pltpu.make_async_copy(source, target, sems.at[at])
        for at, (source, target) in enumerate(zip(sources, targets))
    ]
    for move in moves:
        move.start()
    moves[0].wait()
    moves[1].wait()
    level_total, width = diag_ref.shape[0], diag_ref.shape[-1]
    inverses = invert_lower([diag_ref[level, 0, 0] for level in range(level_total)])
    solved = mm_nt(right_ref[0, 0, 0], inverses[0])
    solved_ref[...] = solved
    at = Layout(level_total, *right_ref.shape[3:], table_refs[0].shape[2])
    packed_ref[at.solved : at.right] = solved
    for tier in range(level_total - 1):
        packed_ref[tier * width : (tier + 1) * width] = inverses[tier + 1]
        begin = at.right + tier * at.width_rhs
        packed_ref[begin : begin + at.width_rhs] = right_ref[tier + 1, 0, 0]
    packed_ref[at.tables : at.rows] = jnp.zeros((at.rows - at.tables, width), jnp.float32)
    for move in moves[2:-1]:
        move.wait()
    for table, ref in enumerate(table_refs[:3]):
        begin = at.tables + table * at.tiers
        packed_ref[begin : begin + at.tiers, : ref.shape[3]] = ref[0, 0].astype(jnp.float32)
    begin = at.tables + 3 * at.tiers
    packed_ref[begin : begin + 1, : at.tiers] = table_refs[3][0].astype(jnp.float32)
    moves[-1].wait()


class Layout:
    def __init__(self, level_total, width_rhs, width, tiers):
        self.width_rhs, self.width, self.tiers = width_rhs, width, tiers
        self.solved = (level_total - 1) * width
        self.right = self.solved + width_rhs
        self.tables = self.right + (level_total - 1) * width_rhs
        self.rows = self.tables + 4 * tiers

    def half(self, begin, me):
        size = self.width_rhs // 2
        return pl.ds(pl.multiple_of(begin + me * size, size), size)


def copy_to_all(copies_ref, row, value):
    for peer in range(copies_ref.shape[0]):
        copies_ref[peer, row] = value


def spread_kernel(at, both_ref, copies_ref, spent_ref):
    me = lax.axis_index("core")
    steps = jnp.where(me == 1, HEAD_START, 0)
    spent_ref[0] = lax.fori_loop(0, steps, lambda i, v: v * 5 + i, me)
    for row in range(2):
        copy_to_all(copies_ref, row, both_ref[row, at.half(at.solved, me)])


def reduced_solve(at, level, received_ref, both_ref):
    me = lax.axis_index("core")
    total = received_ref[0]
    for peer in range(1, received_ref.shape[0]):
        total = total + received_ref[peer]
    begin = at.right + (level - 1) * at.width_rhs
    inverse = pl.ds((level - 1) * at.width, at.width)
    return [
        mm_nt(both_ref[row, at.half(begin, me)] - total[row], both_ref[row, inverse])
        for row in range(2)
    ]


def solve_kernel(at, level, received_ref, both_ref, solved_ref, copies_ref):
    for row, solved in enumerate(reduced_solve(at, level, received_ref, both_ref)):
        solved_ref[row] = solved
        copy_to_all(copies_ref, row, solved)


def last_kernel(at, received_ref, both_ref, *refs):
    earlier, (mine_ref, other_ref, last_ref) = refs[:-3], refs[-3:]
    me = lax.axis_index("core")
    level = len(earlier) + 1
    for row, solved in enumerate(reduced_solve(at, level, received_ref, both_ref)):
        last_ref[row] = solved
    for tier, ref in enumerate((*earlier, last_ref)):
        mine_ref[tier] = ref[me]
        other_ref[tier] = ref[1 - me]


def join_kernel(solved_ref, mine_ref, traded_ref, out_ref, sems):
    me = lax.axis_index("core")
    tiers, size = mine_ref.shape[:2]

    def half_of(core):
        return out_ref.at[pl.ds(1, tiers), pl.ds(pl.multiple_of(core * size, size), size)]

    moves = [
        pltpu.make_async_copy(solved_ref, out_ref.at[0], sems.at[0]),
        pltpu.make_async_copy(mine_ref, half_of(me), sems.at[1]),
        pltpu.make_async_copy(traded_ref.at[1 - me], half_of(1 - me), sems.at[2]),
    ]
    for move in moves:
        move.start()
    for move in moves:
        move.wait()


def split(value):
    high = value.astype(jnp.bfloat16)
    return high, (value - high.astype(jnp.float32)).astype(jnp.bfloat16)


def product(operand, block):
    rows, columns = operand.shape[0], block.shape[0]
    parts = lax.dot_general(
        jnp.concatenate(split(operand), axis=0),
        jnp.concatenate(split(block), axis=0),
        (((1,), (1,)), ((), ())),
        preferred_element_type=jnp.float32,
    )
    smaller = parts[rows:, :columns] + (parts[:rows, columns:] + parts[rows:, columns:])
    return parts[:rows, :columns] + smaller


def product_kernel(at, tier, both_ref, own_ref, other_ref, *refs):
    gathered, out_ref = refs[:-1], refs[-1]
    slots = own_ref.shape[3]
    out_ref[...] = jnp.zeros_like(out_ref)
    me = lax.axis_index("core")
    found = []
    for row, blocks_ref in ((me, own_ref), (1 - me, other_ref)):
        tables = [both_ref[row, at.tables + table * at.tiers + tier] for table in range(3)]
        targets, source_levels, positions = (table.astype(jnp.int32) for table in tables)
        counts = both_ref[row, at.tables + 3 * at.tiers].astype(jnp.int32)
        for s in range(slots):
            position = positions[s]
            operand = gathered[0][position, row]
            for other in range(1, tier + 1):
                operand = jnp.where(
                    source_levels[s] == other, gathered[other][position, row], operand
                )
            operand = jnp.where(s < counts[tier], operand, 0.0)
            found.append((targets[s], product(operand, blocks_ref[0, 0, tier, s])))
    for target, value in found:
        out_ref[target // 2, target % 2] = out_ref[target // 2, target % 2] + value


def call(kernel, outs, in_spaces, name, scratch=()):
    return pl.pallas_call(
        kernel,
        out_shape=outs,
        in_specs=[pl.BlockSpec(memory_space=space) for space in in_spaces],
        out_specs=jax.tree.map(lambda _: pl.BlockSpec(memory_space=VMEM), outs),
        cost_estimate=pl.CostEstimate(flops=1 << 26, bytes_accessed=1 << 20, transcendentals=0),
        scratch_shapes=scratch,
        compiler_params=pltpu.CompilerParams(vmem_limit_bytes=GRANT),
        name=name,
    )


def per_device(
    right_side, diag_blocks, off_blocks, slot_target, slot_level, slot_position, slot_count
):
    level_total, _, _, width_rhs, width = right_side.shape
    tiers = level_total - 1
    at = Layout(level_total, width_rhs, width, tiers)
    half = (width_rhs // 2, width)

    def shape(*dims):
        return jax.ShapeDtypeStruct(dims, jnp.float32)

    solved_shape = shape(2, *half)
    copies_shape = shape(lax.axis_size("col"), 2, *half)
    partial_shape = shape(lax.axis_size("chip"), 2, *half)
    part_shape = shape(tiers, *half)
    inputs = (
        diag_blocks, right_side, off_blocks, slot_target, slot_level, slot_position, slot_count
    )

    packed, first_solved, own_blocks = call(
        first_kernel,
        (shape(at.rows, width), shape(width_rhs, width), shape(*off_blocks.shape)),
        (pltpu.HBM,) * 7,
        "first",
        (
            *(pltpu.VMEM(x.shape, x.dtype) for x in inputs[:2] + inputs[3:]),
            pltpu.SemaphoreType.DMA((7,)),
        ),
    )(*(pltpu.with_memory_space_constraint(x, pltpu.HBM) for x in inputs))
    other_blocks = lax.ppermute(off_blocks, "core", [(0, 1), (1, 0)])
    both = lax.all_gather(packed, "core", axis=0, tiled=False)
    copies = call(
        functools.partial(spread_kernel, at),
        copies_shape,
        (VMEM,),
        "spread",
        (pltpu.SMEM((1,), jnp.int32),),
    )(both)
    results, gathered = [], []
    for level in range(1, level_total):
        gathered.append(lax.all_to_all(copies, "col", 0, 0, tiled=True))
        partial = call(
            functools.partial(product_kernel, at, level - 1),
            partial_shape,
            (VMEM,) * (3 + level),
            "products",
        )(both, own_blocks, other_blocks, *gathered)
        received = lax.all_to_all(partial, "chip", 0, 0, tiled=True)
        if level + 1 < level_total:
            solved, copies = call(
                functools.partial(solve_kernel, at, level),
                (solved_shape, copies_shape),
                (VMEM,) * 2,
                "solve",
            )(received, both)
            results.append(solved)
    mine, other = call(
        functools.partial(last_kernel, at),
        (part_shape, part_shape),
        (VMEM,) * (2 + len(results)),
        "last",
        (pltpu.VMEM((2, *half), jnp.float32),),
    )(received, both, *results)
    traded = lax.all_gather(other, "core", axis=0, tiled=False)
    out = pl.pallas_call(
        join_kernel,
        out_shape=shape(level_total, width_rhs, width),
        in_specs=[pl.BlockSpec(memory_space=VMEM)] * 3,
        out_specs=pl.BlockSpec(memory_space=pltpu.HBM),
        scratch_shapes=(pltpu.SemaphoreType.DMA((3,)),),
        compiler_params=pltpu.CompilerParams(vmem_limit_bytes=GRANT),
        name="join",
    )(first_solved, mine, traded)
    return out[:, None, None]


def solution(mesh):
    rows, cols = mesh.shape["row"], mesh.shape["col"]
    fine = Mesh(mesh.devices.reshape(rows // 2, 2, cols), ("chip", "core", "col"))
    row, col = ("chip", "core"), "col"
    placed = (
        P(None, row, col, None, None),
        P(None, row, col, None, None),
        P(row, col, None, None, None, None),
        P(row, col, None, None),
        P(row, col, None, None),
        P(row, col, None, None),
        P(row, col, None),
    )
    return jax.shard_map(
        per_device,
        mesh=fine,
        in_specs=placed,
        out_specs=P(None, row, col, None, None),
        check_vma=False,
    )
```
